8 devices in a mesh: ens: 2 (over z, y), sp: 4 (over x, core).
Axes of the slice: x: 2, y: 2, z: 1, core: 2. Of those that a mesh axis runs over, the one named last changes fastest.
Arguments:
- x_seq: bfloat16 [4096, 512], P(('ens', 'sp')), parts along dimension 0
- w_past: bfloat16 [3, 10, 512, 1024], replicated
- w_now: bfloat16 [3, 10, 512, 1024], replicated
- b_conv: float32 [3, 10, 1024], replicated
- w_res: bfloat16 [3, 10, 512, 512], replicated
- w_skip: bfloat16 [3, 10, 512, 256], replicated
- w_out1: bfloat16 [256, 256], replicated
- b_out1: float32 [256], replicated
- w_out2: bfloat16 [256, 256], replicated
- b_out2: float32 [256], replicated
Outputs:
- output 1: float32 [4096, 256], P(('ens', 'sp')), parts along dimension 0
- output 2: bfloat16 [4096, 512], P(('ens', 'sp')), parts along dimension 0
There are 2 independent parts. The reference program is written for one: setup_inputs(seed, part) draws one part's arguments, and reference() takes and returns one part's arrays. A program takes and returns all parts, laid end to end along the dimension named above; an argument that names none is the same for every part.
All inputs are finite; a program needn't handle non-finite values.
Results may differ from the reference program's by a relative error of at most 0.02.
Values are sent between devices in bfloat16 or wider.
A program may use at most 1 GiB of HBM per device.

```python
import jax
import jax.numpy as jnp
from jax import lax

SEQ_LEN = 2048
RES_CH = 512
GATE_CH = 512
SKIP_CH = 256
CLASSES = 256
DIL_CYCLE = 10
STACKS = 3
LAYERS_ALL = STACKS * DIL_CYCLE


def setup_inputs(seed: int = 0, part: int = 0) -> dict:
    root_key = jax.random.key(seed)
    subkeys = jax.random.split(root_key, 10)
    seq_key = jax.random.fold_in(subkeys[0], part)
    conv_shape = (STACKS, DIL_CYCLE, RES_CH, 2 * GATE_CH)
    conv_scale = (2 * RES_CH) ** -0.5
    proj_scale = 2.0 * (GATE_CH * LAYERS_ALL) ** -0.5
    head_scale = 2.0 * SKIP_CH ** -0.5
    x_seq = jax.random.normal(seq_key, (SEQ_LEN, RES_CH), jnp.float32)
    w_past = jax.random.normal(subkeys[1], conv_shape, jnp.float32) * conv_scale
    w_now = jax.random.normal(subkeys[2], conv_shape, jnp.float32) * conv_scale
    b_conv = jax.random.normal(subkeys[3], (STACKS, DIL_CYCLE, 2 * GATE_CH), jnp.float32) * 0.5
    w_res = jax.random.normal(subkeys[4], (STACKS, DIL_CYCLE, GATE_CH, RES_CH), jnp.float32) * proj_scale
    w_skip = jax.random.normal(subkeys[5], (STACKS, DIL_CYCLE, GATE_CH, SKIP_CH), jnp.float32) * proj_scale
    w_out1 = jax.random.normal(subkeys[6], (SKIP_CH, SKIP_CH), jnp.float32) * head_scale
    b_out1 = jax.random.normal(subkeys[7], (SKIP_CH,), jnp.float32) * 0.5
    w_out2 = jax.random.normal(subkeys[8], (SKIP_CH, CLASSES), jnp.float32) * head_scale
    b_out2 = jax.random.normal(subkeys[9], (CLASSES,), jnp.float32) * 0.5
    return {
        "x_seq": x_seq.astype(jnp.bfloat16),
        "w_past": w_past.astype(jnp.bfloat16),
        "w_now": w_now.astype(jnp.bfloat16),
        "b_conv": b_conv,
        "w_res": w_res.astype(jnp.bfloat16),
        "w_skip": w_skip.astype(jnp.bfloat16),
        "w_out1": w_out1.astype(jnp.bfloat16),
        "b_out1": b_out1,
        "w_out2": w_out2.astype(jnp.bfloat16),
        "b_out2": b_out2,
    }


def reference(x_seq, w_past, w_now, b_conv, w_res, w_skip, w_out1, b_out1, w_out2, b_out2):
    def stack_body(carry, stack_w):
        hidden, skip_sum = carry
        past_w, now_w, conv_b, res_w, skip_w = stack_w
        for layer_pos in range(DIL_CYCLE):
            dilation = 2 ** layer_pos
            shifted = jnp.concatenate([jnp.zeros((dilation, RES_CH), hidden.dtype), hidden[:SEQ_LEN - dilation]], axis=0)
            pre_act = (jnp.dot(shifted, past_w[layer_pos], preferred_element_type=jnp.float32)
                       + jnp.dot(hidden, now_w[layer_pos], preferred_element_type=jnp.float32)
                       + conv_b[layer_pos])
            gated = (jnp.tanh(pre_act[:, :GATE_CH]) * jax.nn.sigmoid(pre_act[:, GATE_CH:])).astype(jnp.bfloat16)
            hidden = (hidden.astype(jnp.float32) + jnp.dot(gated, res_w[layer_pos], preferred_element_type=jnp.float32)).astype(jnp.bfloat16)
            skip_sum = skip_sum + jnp.dot(gated, skip_w[layer_pos], preferred_element_type=jnp.float32)
        return (hidden, skip_sum), None

    skip_init = jnp.zeros((SEQ_LEN, SKIP_CH), jnp.float32)
    (hidden, skip_sum), _ = lax.scan(stack_body, (x_seq, skip_init), (w_past, w_now, b_conv, w_res, w_skip))
    skip_act = jax.nn.relu(skip_sum).astype(jnp.bfloat16)
    mid_act = jax.nn.relu(jnp.dot(skip_act, w_out1, preferred_element_type=jnp.float32) + b_out1).astype(jnp.bfloat16)
    logits = jnp.dot(mid_act, w_out2, preferred_element_type=jnp.float32) + b_out2
    return (logits, hidden)
```

```python
import functools

import jax
import jax.numpy as jnp
from jax import lax
from jax.experimental import pallas as pl
from jax.experimental.pallas import tpu as pltpu
from jax.sharding import PartitionSpec as P

TILE = 16
SLOTS = 5
STATIC = 4


def _kernel(n_sp, repeats, cycle, rows, x_ref, wp_ref, wn_ref, b_ref, wr_ref, ws_ref, w1_ref, c1_ref, w2_ref, c2_ref,
            y_ref, h_ref, hb, g_s, skip, wpb, wnb, wrb, wsb, wsem, xsem, osem, send_sem, recv_sem):
    me = lax.axis_index("sp")
    layers = repeats * cycle
    ch = x_ref.shape[1]
    gate = wn_ref.shape[2] // 2
    pads = [max(TILE, 2 ** k) for k in range(cycle)]
    stack_rows = sum(pads) + cycle * rows

    def base_of(s, k):
        return s * stack_rows + sum(pads[:k]) + k * rows

    def weight_copies(layer, slot):
        pairs = ((wp_ref, wpb), (wn_ref, wnb), (wr_ref, wrb), (ws_ref, wsb))
        return [pltpu.make_async_copy(src.at[layer], dst.at[slot], wsem.at[slot, i]) for i, (src, dst) in enumerate(pairs)]

    def halo_copy(s, base, k, pad):
        return pltpu.make_async_remote_copy(
            src_ref=hb.at[pl.ds(pl.multiple_of(base + rows, TILE), pad), :],
            dst_ref=hb.at[pl.ds(pl.multiple_of(base, TILE), pad), :],
            send_sem=send_sem.at[s, k], recv_sem=recv_sem.at[s, k],
            device_id={"sp": jnp.minimum(me + 1, n_sp - 1)}, device_id_type=pl.DeviceIdType.MESH)

    x_copy = pltpu.make_async_copy(x_ref, hb.at[pl.ds(pads[0], rows), :], xsem)
    x_copy.start()
    for slot in range(SLOTS - 1):
        for c in weight_copies(slot, slot):
            c.start()
    barrier = pltpu.get_barrier_semaphore()

    @pl.when(me > 0)
    def _():
        pl.semaphore_signal(barrier, inc=1, device_id={"sp": me - 1}, device_id_type=pl.DeviceIdType.MESH)

    @pl.when(me == 0)
    def _():
        for s in range(repeats):
            for k in range(cycle):
                hb[base_of(s, k):base_of(s, k) + pads[k], :] = jnp.zeros((pads[k], ch), hb.dtype)

    skip[...] = jnp.zeros_like(skip)

    @pl.when(me < n_sp - 1)
    def _():
        pl.semaphore_wait(barrier, 1)

    x_copy.wait()

    def layer_body(s, k, base, pad, next_local, static_d):
        layer = s * cycle + k
        slot = lax.rem(layer, SLOTS)
        local = pl.multiple_of(base + pad, TILE)
        if static_d is not None:
            @pl.when(me < n_sp - 1)
            def _():
                halo_copy(s, base, k, TILE).start()
        else:
            for kk in range(STATIC, cycle):
                @pl.when((me < n_sp - 1) & (k == kk))
                def _():
                    halo_copy(s, base, k, pads[kk]).start()
        ahead = layer + SLOTS - 1

        @pl.when(ahead < layers)
        def _():
            for c in weight_copies(ahead, lax.rem(ahead, SLOTS)):
                c.start()
        for c in weight_copies(layer, slot):
            c.wait()
        if static_d is not None:
            @pl.when(me > 0)
            def _():
                halo_copy(s, base, k, TILE).wait_recv()
        else:
            for kk in range(STATIC, cycle):
                @pl.when((me > 0) & (k == kk))
                def _():
                    halo_copy(s, base, k, pads[kk]).wait_recv()
        here = hb[pl.ds(local, rows), :]
        if static_d is not None:
            past = hb[pl.ds(local - TILE, rows + TILE), :][TILE - static_d:TILE - static_d + rows, :]
        else:
            past = hb[pl.ds(pl.multiple_of(base, TILE), rows), :]
        half = gate // 2
        for j in range(2):
            def pre(col):
                return (jnp.dot(past, wpb[slot, :, col:col + half], preferred_element_type=jnp.float32)
                        + jnp.dot(here, wnb[slot, :, col:col + half], preferred_element_type=jnp.float32)
                        + b_ref[pl.ds(layer, 1), col:col + half])
            a = jnp.tanh(pre(j * half))
            t = jnp.tanh(0.5 * pre(gate + j * half))
            g_s[:, j * half:(j + 1) * half] = (a * (0.5 * t + 0.5)).astype(jnp.bfloat16)
        g = g_s[...]
        new = here.astype(jnp.float32) + jnp.dot(g, wrb[slot], preferred_element_type=jnp.float32)
        hb[pl.ds(pl.multiple_of(next_local, TILE), rows), :] = new.astype(hb.dtype)
        skip[...] += jnp.dot(g, wsb[slot], preferred_element_type=jnp.float32)

    def stack(s, carry):
        for k in range(STATIC):
            nxt = base_of(s, k + 1) + pads[k + 1]
            layer_body(s, k, base_of(s, k), pads[k], nxt, 2 ** k)

        def wide(k, carry):
            base, pad = carry
            last = k == cycle - 1
            next_base = base + pad + rows
            next_pad = jnp.where(last, pads[0], 2 * pad)
            layer_body(s, k, base, pad, next_base + next_pad, None)
            return next_base, next_pad

        lax.fori_loop(STATIC, cycle, wide, (base_of(s, STATIC), jnp.int32(pads[STATIC])))
        return carry

    lax.fori_loop(0, repeats, stack, 0)

    final = repeats * stack_rows + pads[0]
    out_copy = pltpu.make_async_copy(hb.at[pl.ds(final, rows), :], h_ref, osem)
    out_copy.start()
    act = jnp.maximum(skip[...], 0.0).astype(jnp.bfloat16)
    mid = jnp.dot(act, w1_ref[...], preferred_element_type=jnp.float32) + c1_ref[...]
    mid = jnp.maximum(mid, 0.0).astype(jnp.bfloat16)
    y_ref[...] = jnp.dot(mid, w2_ref[...], preferred_element_type=jnp.float32) + c2_ref[...]
    out_copy.wait()

    @pl.when(me < n_sp - 1)
    def _():
        for s in range(repeats):
            for k in range(cycle):
                halo_copy(s, base_of(s, k), k, pads[k]).wait_send()


def solution(mesh):
    n_sp = mesh.shape["sp"]
    row_spec = P(("ens", "sp"), None)

    def local_stack(x_seq, w_past, w_now, b_conv, w_res, w_skip, w_out1, b_out1, w_out2, b_out2):
        repeats, cycle, ch, wide = w_past.shape
        layers, rows = repeats * cycle, x_seq.shape[0]
        gate, skips = w_res.shape[2], w_skip.shape[3]
        classes = w_out2.shape[1]
        pads = [max(TILE, 2 ** k) for k in range(cycle)]
        region = repeats * (sum(pads) + cycle * rows) + pads[0] + rows
        hbm = pl.BlockSpec(memory_space=pltpu.HBM)
        vmem = pl.BlockSpec(memory_space=pltpu.VMEM)
        return pl.pallas_call(
            functools.partial(_kernel, n_sp, repeats, cycle, rows),
            name="stack",
            out_shape=(jax.ShapeDtypeStruct((rows, classes), jnp.float32), jax.ShapeDtypeStruct((rows, ch), x_seq.dtype)),
            in_specs=[hbm, hbm, hbm, vmem, hbm, hbm, vmem, vmem, vmem, vmem],
            out_specs=(vmem, hbm),
            scratch_shapes=[
                pltpu.VMEM((region, ch), x_seq.dtype),
                pltpu.VMEM((rows, gate), jnp.bfloat16),
                pltpu.VMEM((rows, skips), jnp.float32),
                pltpu.VMEM((SLOTS, ch, wide), w_past.dtype),
                pltpu.VMEM((SLOTS, ch, wide), w_now.dtype),
                pltpu.VMEM((SLOTS, gate, ch), w_res.dtype),
                pltpu.VMEM((SLOTS, gate, skips), w_skip.dtype),
                pltpu.SemaphoreType.DMA((SLOTS, 4)),
                pltpu.SemaphoreType.DMA,
                pltpu.SemaphoreType.DMA,
                pltpu.SemaphoreType.DMA((repeats, cycle)),
                pltpu.SemaphoreType.DMA((repeats, cycle)),
            ],
            compiler_params=pltpu.CompilerParams(collective_id=0, has_side_effects=True, vmem_limit_bytes=60 * 2 ** 20),
        )(x_seq, w_past.reshape(layers, ch, wide), w_now.reshape(layers, ch, wide), b_conv.reshape(layers, wide),
          w_res.reshape(layers, gate, ch), w_skip.reshape(layers, gate, skips),
          w_out1, b_out1.reshape(1, -1), w_out2, b_out2.reshape(1, -1))

    return jax.shard_map(
        local_stack,
        mesh=mesh,
        in_specs=(row_spec, P(), P(), P(), P(), P(), P(), P(), P(), P()),
        out_specs=(row_spec, row_spec),
        check_vma=False,
    )
```

```python
import functools

import jax
import jax.numpy as jnp
from jax import lax
from jax.experimental import pallas as pl
from jax.experimental.pallas import tpu as pltpu
from jax.sharding import PartitionSpec as P

TILE = 16
SLOTS = 5
SIDE = 256
BLOCK = 128


_STAGED = {}
_LOADED = {}


def push_rhs(w, staging_register, mxu_index):
    _STAGED[(mxu_index, staging_register)] = w


def acc_lhs(acc, lhs, load_staged_rhs, q):
    if load_staged_rhs is not None:
        _LOADED[q] = _STAGED[(q, load_staged_rhs)]
    acc[...] += jnp.dot(lhs, _LOADED[q], preferred_element_type=jnp.float32)


def pop(acc):
    v = acc[...]
    acc[...] = jnp.zeros_like(v)
    return v


def _kernel(n_sp, repeats, cycle, rows, x_ref, wp_ref, wn_ref, b_ref, wr_ref, ws_ref,
            skip, h_ref, hb, ps, g_s, wpb, wnb, wrb, wsb, wsem, xsem, osem, send_sem, recv_sem):
    me = lax.axis_index("sp")
    layers = repeats * cycle
    ch = x_ref.shape[1]
    gate = wn_ref.shape[2] // 2
    nb = rows // BLOCK
    pads = [max(TILE, 2 ** k) for k in range(cycle)]
    stack_rows = sum(pads) + cycle * rows

    def base_of(s, k):
        return s * stack_rows + sum(pads[:k]) + k * rows

    def local_of(s, k):
        return base_of(s, k) + pads[k % cycle]

    def weight_copies(layer, slot):
        pairs = ((wp_ref, wpb), (wn_ref, wnb), (wr_ref, wrb), (ws_ref, wsb))
        return [pltpu.make_async_copy(src.at[layer], dst.at[slot], wsem.at[slot, i]) for i, (src, dst) in enumerate(pairs)]

    def halo_copy(s, k):
        base = base_of(s, k)
        return pltpu.make_async_remote_copy(
            src_ref=hb.at[pl.ds(pl.multiple_of(base + rows, TILE), pads[k]), :],
            dst_ref=hb.at[pl.ds(pl.multiple_of(base, TILE), pads[k]), :],
            send_sem=send_sem.at[s, k], recv_sem=recv_sem.at[s, k],
            device_id={"sp": jnp.minimum(me + 1, n_sp - 1)}, device_id_type=pl.DeviceIdType.MESH)

    def at(start, size):
        return pl.ds(pl.multiple_of(start, TILE), size)

    def body(acc0, acc1):
        X = (acc0[:nb], acc1[:nb])
        Y = (acc0[nb:], acc1[nb:])

        def steps_of(s, k):
            slot = k % SLOTS
            local = local_of(s, k)
            d = 2 ** (k % cycle)

            def here(kt):
                return lambda q, i: hb[at(local + i * BLOCK, BLOCK), kt * SIDE:(kt + 1) * SIDE]

            def past(kt):
                if d < TILE:
                    return lambda q, i: ps[i * BLOCK:(i + 1) * BLOCK, kt * SIDE:(kt + 1) * SIDE]
                return lambda q, i: hb[at(local - d + i * BLOCK, BLOCK), kt * SIDE:(kt + 1) * SIDE]

            def gated(kt):
                return lambda q, i: g_s[i * BLOCK:(i + 1) * BLOCK, kt * SIDE:(kt + 1) * SIDE]

            def gated_half(kt):
                return lambda q, i: g_s[q * (rows // 2) + i * BLOCK:q * (rows // 2) + (i + 1) * BLOCK, kt * SIDE:(kt + 1) * SIDE]

            def w(buf, kt, col):
                return lambda q: buf[slot, kt * SIDE:(kt + 1) * SIDE, col(q):col(q) + SIDE]

            out = []
            for acc, j in ((X, 0), (Y, 1)):
                out += [(w(wnb, kt, lambda q, j=j: q * gate + j * SIDE), here(kt), acc, nb) for kt in range(2)]
            for acc, j in ((X, 0), (Y, 1)):
                out += [(w(wpb, kt, lambda q, j=j: q * gate + j * SIDE), past(kt), acc, nb) for kt in range(2)]
            out += [(w(wrb, kt, lambda q: q * SIDE), gated(kt), X, nb) for kt in range(2)]
            out += [(w(wsb, kt, lambda q: 0), gated_half(kt), Y, nb // 2) for kt in range(2)]
            return out

        def push(step, n):
            for q in range(2):
                push_rhs(step[0](q), staging_register=n % 2, mxu_index=q)

        def run(step, following, n):
            for i in range(step[3]):
                for q in range(2):
                    acc_lhs(step[2][q][i], step[1](q, i), n % 2 if i == 0 else None, q)
                if i == 0:
                    push(following, n + 1)

        def gate_half(s, k, acc, j):
            ba = b_ref[k, pl.ds(s, 1), j * SIDE:(j + 1) * SIDE]
            bt = b_ref[k, pl.ds(s, 1), gate + j * SIDE:gate + (j + 1) * SIDE]
            for i in range(nb):
                a = jnp.tanh(pop(acc[0][i]) + ba)
                t = jnp.tanh(0.5 * (pop(acc[1][i]) + bt))
                g_s[i * BLOCK:(i + 1) * BLOCK, j * SIDE:(j + 1) * SIDE] = (a * (0.5 * t + 0.5)).astype(jnp.bfloat16)

        def take_skip():
            for q in range(2):
                for i in range(nb // 2):
                    lo = q * (rows // 2) + i * BLOCK
                    skip[lo:lo + BLOCK, :] += pop(Y[q][i])

        def take_res(s, k):
            old, new = local_of(s, k), local_of(s, k + 1)
            for i in range(nb):
                for q in range(2):
                    cols = slice(q * SIDE, (q + 1) * SIDE)
                    v = hb[at(old + i * BLOCK, BLOCK), cols].astype(jnp.float32) + pop(X[q][i])
                    hb[at(new + i * BLOCK, BLOCK), cols] = v.astype(hb.dtype)

        for q in range(2):
            for i in range(nb):
                X[q][i][...] = jnp.zeros_like(X[q][i])
                Y[q][i][...] = jnp.zeros_like(Y[q][i])
        for c in weight_copies(0, 0):
            c.wait()
        x_copy.wait()
        first = steps_of(0, 0)
        push(first[0], 0)
        run(first[0], first[1], 0)

        def stack(s, carry):
            push(steps_of(s, 0)[1], 1)
            for k in range(cycle):
                layer = s * cycle + k
                st = steps_of(s, k)
                nxt = steps_of(s, k + 1)
                d = 2 ** k

                @pl.when(me < n_sp - 1)
                def _():
                    halo_copy(s, k).start()

                def fetch():
                    for c in weight_copies(layer + SLOTS - 1, (k + SLOTS - 1) % SLOTS):
                        c.start()

                def arrive():
                    for c in weight_copies(layer + 1, (k + 1) % SLOTS):
                        c.wait()
                if k + SLOTS - 1 < cycle:
                    fetch()
                else:
                    pl.when(s < repeats - 1)(fetch)
                if k + 1 < cycle:
                    arrive()
                else:
                    pl.when(s < repeats - 1)(arrive)
                take_skip()
                run(st[1], st[2], 1)
                local = local_of(s, k)
                if d < TILE:
                    ps[TILE:rows, :] = hb[at(local, rows), :][TILE - d:rows - d, :]
                run(st[2], st[3], 2)
                run(st[3], st[4], 3)

                @pl.when(me > 0)
                def _():
                    halo_copy(s, k).wait_recv()
                if d < TILE:
                    ps[0:TILE, :] = hb[at(local - TILE, 2 * TILE), :][TILE - d:2 * TILE - d, :]
                run(st[4], st[5], 4)
                run(st[5], st[6], 5)
                gate_half(s, k, X, 0)
                run(st[6], st[7], 6)
                run(st[7], st[8], 7)
                gate_half(s, k, Y, 1)
                run(st[8], st[9], 8)
                run(st[9], st[10], 9)
                run(st[10], st[11], 10)
                run(st[11], nxt[0], 11)
                take_res(s, k)
                run(nxt[0], nxt[1], 12)
            return carry

        lax.fori_loop(0, repeats, stack, 0)
        take_skip()
        for q in range(2):
            pass
            for i in range(nb):
                pop(X[q][i])

    x_copy = pltpu.make_async_copy(x_ref, hb.at[pl.ds(pads[0], rows), :], xsem)
    x_copy.start()
    for slot in range(SLOTS - 1):
        for c in weight_copies(slot, slot):
            c.start()
    barrier = pltpu.get_barrier_semaphore()

    @pl.when(me > 0)
    def _():
        pl.semaphore_signal(barrier, inc=1, device_id={"sp": me - 1}, device_id_type=pl.DeviceIdType.MESH)

    @pl.when(me == 0)
    def _():
        for s in range(repeats):
            for k in range(cycle):
                hb[base_of(s, k):base_of(s, k) + pads[k], :] = jnp.zeros((pads[k], ch), hb.dtype)

    skip[...] = jnp.zeros_like(skip)

    @pl.when(me < n_sp - 1)
    def _():
        pl.semaphore_wait(barrier, 1)

    specs = tuple(pltpu.VMEM((BLOCK, SIDE), jnp.float32) for q in range(2) for _ in range(2 * nb))
    pl.run_scoped(lambda *refs: body(refs[:2 * nb], refs[2 * nb:]), *specs)

    out_copy = pltpu.make_async_copy(hb.at[pl.ds(local_of(repeats - 1, cycle), rows), :], h_ref, osem)
    out_copy.start()
    out_copy.wait()

    @pl.when(me < n_sp - 1)
    def _():
        for s in range(repeats):
            for k in range(cycle):
                halo_copy(s, k).wait_send()


def _head(skip, h_ref, w1_ref, c1_ref, w2_ref, c2_ref, y_ref, out_ref):
    out_ref[...] = h_ref[...]
    act = jnp.maximum(skip[...], 0.0).astype(jnp.bfloat16)
    mid = jnp.dot(act, w1_ref[...], preferred_element_type=jnp.float32) + c1_ref[...]
    mid = jnp.maximum(mid, 0.0).astype(jnp.bfloat16)
    y_ref[...] = jnp.dot(mid, w2_ref[...], preferred_element_type=jnp.float32) + c2_ref[...]


def solution(mesh):
    n_sp = mesh.shape["sp"]
    row_spec = P(("ens", "sp"), None)

    def local_stack(x_seq, w_past, w_now, b_conv, w_res, w_skip, w_out1, b_out1, w_out2, b_out2):
        repeats, cycle, ch, wide = w_past.shape
        layers, rows = repeats * cycle, x_seq.shape[0]
        gate, skips = w_res.shape[2], w_skip.shape[3]
        classes = w_out2.shape[1]
        pads = [max(TILE, 2 ** k) for k in range(cycle)]
        region = repeats * (sum(pads) + cycle * rows) + pads[0] + rows
        hbm = pl.BlockSpec(memory_space=pltpu.HBM)
        vmem = pl.BlockSpec(memory_space=pltpu.VMEM)
        anywhere = pl.BlockSpec(memory_space=pl.ANY)
        skip, h = pl.pallas_call(
            functools.partial(_kernel, n_sp, repeats, cycle, rows),
            name="stack",
            out_shape=(jax.ShapeDtypeStruct((rows, skips), jnp.float32), jax.ShapeDtypeStruct((rows, ch), x_seq.dtype)),
            in_specs=[hbm, hbm, hbm, vmem, hbm, hbm],
            out_specs=(vmem, anywhere),
            scratch_shapes=[
                pltpu.VMEM((region, ch), x_seq.dtype),
                pltpu.VMEM((rows, ch), x_seq.dtype),
                pltpu.VMEM((rows, gate), jnp.bfloat16),
                pltpu.VMEM((SLOTS, ch, wide), w_past.dtype),
                pltpu.VMEM((SLOTS, ch, wide), w_now.dtype),
                pltpu.VMEM((SLOTS, gate, ch), w_res.dtype),
                pltpu.VMEM((SLOTS, gate, skips), w_skip.dtype),
                pltpu.SemaphoreType.DMA((SLOTS, 4)),
                pltpu.SemaphoreType.DMA,
                pltpu.SemaphoreType.DMA,
                pltpu.SemaphoreType.DMA((repeats, cycle)),
                pltpu.SemaphoreType.DMA((repeats, cycle)),
            ],
            compiler_params=pltpu.CompilerParams(collective_id=0, has_side_effects=True, vmem_limit_bytes=46 * 2 ** 20),
        )(x_seq, w_past.reshape(layers, ch, wide), w_now.reshape(layers, ch, wide), jnp.transpose(b_conv, (1, 0, 2)),
          w_res.reshape(layers, gate, ch), w_skip.reshape(layers, gate, skips))
        return pl.pallas_call(
            _head,
            name="head",
            out_shape=(jax.ShapeDtypeStruct((rows, classes), jnp.float32), jax.ShapeDtypeStruct((rows, ch), x_seq.dtype)),
            in_specs=[vmem] * 6,
            out_specs=(vmem, vmem),
        )(skip, h, w_out1, b_out1.reshape(1, -1), w_out2, b_out2.reshape(1, -1))

    return jax.shard_map(
        local_stack,
        mesh=mesh,
        in_specs=(row_spec, P(), P(), P(), P(), P(), P(), P(), P(), P()),
        out_specs=(row_spec, row_spec),
        check_vma=False,
    )
```

```python
import functools

import jax
import jax.numpy as jnp
from jax import lax
from jax.experimental import pallas as pl
from jax.experimental.pallas import tpu as pltpu
from jax.sharding import PartitionSpec as P

TILE = 16
SLOTS = 5
SIDE = 256
BLOCK = 128


def _kernel(n_sp, repeats, cycle, rows, x_ref, wp_ref, wn_ref, b_ref, wr_ref, ws_ref,
            skip, h_ref, hb, ps, g_s, wpb, wnb, wrb, wsb, wsem, xsem, osem, send_sem, recv_sem):
    me = lax.axis_index("sp")
    layers = repeats * cycle
    ch = x_ref.shape[1]
    gate = wn_ref.shape[2] // 2
    nb = rows // BLOCK
    pads = [max(TILE, 2 ** k) for k in range(cycle)]
    stack_rows = sum(pads) + cycle * rows

    def base_of(s, k):
        return s * stack_rows + sum(pads[:k]) + k * rows

    def local_of(s, k):
        return base_of(s, k) + pads[k % cycle]

    def weight_copies(layer, slot):
        pairs = ((wp_ref, wpb), (wn_ref, wnb), (wr_ref, wrb), (ws_ref, wsb))
        return [pltpu.make_async_copy(src.at[layer], dst.at[slot], wsem.at[slot, i]) for i, (src, dst) in enumerate(pairs)]

    def halo_copy(s, k):
        base = base_of(s, k)
        return pltpu.make_async_remote_copy(
            src_ref=hb.at[pl.ds(pl.multiple_of(base + rows, TILE), pads[k]), :],
            dst_ref=hb.at[pl.ds(pl.multiple_of(base, TILE), pads[k]), :],
            send_sem=send_sem.at[s, k], recv_sem=recv_sem.at[s, k],
            device_id={"sp": jnp.minimum(me + 1, n_sp - 1)}, device_id_type=pl.DeviceIdType.MESH)

    def at(start, size):
        return pl.ds(pl.multiple_of(start, TILE), size)

    def stack(s, carry):
        for k in range(cycle):
            layer, slot, d = s * cycle + k, k % SLOTS, 2 ** k
            local, new = local_of(s, k), local_of(s, k + 1)

            @pl.when(me < n_sp - 1)
            def _():
                halo_copy(s, k).start()

            def fetch():
                for c in weight_copies(layer + SLOTS - 1, (k + SLOTS - 1) % SLOTS):
                    c.start()
            if k + SLOTS - 1 < cycle:
                fetch()
            else:
                pl.when(s < repeats - 1)(fetch)
            for c in weight_copies(layer, slot):
                c.wait()

            @pl.when(me > 0)
            def _():
                halo_copy(s, k).wait_recv()
            here = hb[at(local, rows), :]
            if d < TILE:
                past = hb[at(local - TILE, rows + TILE), :][TILE - d:TILE - d + rows, :]
            else:
                past = hb[at(local - d, rows), :]
            for j in range(gate // SIDE):
                ca, ct = j * SIDE, gate + j * SIDE

                def both(buf):
                    return jnp.concatenate([buf[slot, :, ca:ca + SIDE], buf[slot, :, ct:ct + SIDE]], axis=1)
                z = (jnp.dot(past, both(wpb), preferred_element_type=jnp.float32)
                     + jnp.dot(here, both(wnb), preferred_element_type=jnp.float32))
                a = jnp.tanh(z[:, :SIDE] + b_ref[k, pl.ds(s, 1), ca:ca + SIDE])
                t = jnp.tanh(0.5 * (z[:, SIDE:] + b_ref[k, pl.ds(s, 1), ct:ct + SIDE]))
                g_s[:, ca:ca + SIDE] = (a * (0.5 * t + 0.5)).astype(jnp.bfloat16)
            g = g_s[...]
            res = here.astype(jnp.float32) + jnp.dot(g, wrb[slot], preferred_element_type=jnp.float32)
            hb[at(new, rows), :] = res.astype(hb.dtype)
            half = rows // 2
            for q in range(2):
                skip[q * half:(q + 1) * half, :] += jnp.dot(g[q * half:(q + 1) * half, :], wsb[slot], preferred_element_type=jnp.float32)
        return carry

    x_copy = pltpu.make_async_copy(x_ref, hb.at[pl.ds(pads[0], rows), :], xsem)
    x_copy.start()
    for slot in range(SLOTS - 1):
        for c in weight_copies(slot, slot):
            c.start()
    barrier = pltpu.get_barrier_semaphore()

    @pl.when(me > 0)
    def _():
        pl.semaphore_signal(barrier, inc=1, device_id={"sp": me - 1}, device_id_type=pl.DeviceIdType.MESH)

    @pl.when(me == 0)
    def _():
        for s in range(repeats):
            for k in range(cycle):
                hb[base_of(s, k):base_of(s, k) + pads[k], :] = jnp.zeros((pads[k], ch), hb.dtype)

    skip[...] = jnp.zeros_like(skip)

    @pl.when(me < n_sp - 1)
    def _():
        pl.semaphore_wait(barrier, 1)

    x_copy.wait()
    lax.fori_loop(0, repeats, stack, 0)

    out_copy = pltpu.make_async_copy(hb.at[pl.ds(local_of(repeats - 1, cycle), rows), :], h_ref, osem)
    out_copy.start()
    out_copy.wait()

    @pl.when(me < n_sp - 1)
    def _():
        for s in range(repeats):
            for k in range(cycle):
                halo_copy(s, k).wait_send()


def _head(skip, h_ref, w1_ref, c1_ref, w2_ref, c2_ref, y_ref, out_ref):
    out_ref[...] = h_ref[...]
    act = jnp.maximum(skip[...], 0.0).astype(jnp.bfloat16)
    mid = jnp.dot(act, w1_ref[...], preferred_element_type=jnp.float32) + c1_ref[...]
    mid = jnp.maximum(mid, 0.0).astype(jnp.bfloat16)
    y_ref[...] = jnp.dot(mid, w2_ref[...], preferred_element_type=jnp.float32) + c2_ref[...]


def solution(mesh):
    n_sp = mesh.shape["sp"]
    row_spec = P(("ens", "sp"), None)

    def local_stack(x_seq, w_past, w_now, b_conv, w_res, w_skip, w_out1, b_out1, w_out2, b_out2):
        repeats, cycle, ch, wide = w_past.shape
        layers, rows = repeats * cycle, x_seq.shape[0]
        gate, skips = w_res.shape[2], w_skip.shape[3]
        classes = w_out2.shape[1]
        pads = [max(TILE, 2 ** k) for k in range(cycle)]
        region = repeats * (sum(pads) + cycle * rows) + pads[0] + rows
        hbm = pl.BlockSpec(memory_space=pltpu.HBM)
        vmem = pl.BlockSpec(memory_space=pltpu.VMEM)
        anywhere = pl.BlockSpec(memory_space=pl.ANY)
        skip, h = pl.pallas_call(
            functools.partial(_kernel, n_sp, repeats, cycle, rows),
            name="stack",
            out_shape=(jax.ShapeDtypeStruct((rows, skips), jnp.float32), jax.ShapeDtypeStruct((rows, ch), x_seq.dtype)),
            in_specs=[hbm, hbm, hbm, vmem, hbm, hbm],
            out_specs=(vmem, anywhere),
            scratch_shapes=[
                pltpu.VMEM((region, ch), x_seq.dtype),
                pltpu.VMEM((rows, ch), x_seq.dtype),
                pltpu.VMEM((rows, gate), jnp.bfloat16),
                pltpu.VMEM((SLOTS, ch, wide), w_past.dtype),
                pltpu.VMEM((SLOTS, ch, wide), w_now.dtype),
                pltpu.VMEM((SLOTS, gate, ch), w_res.dtype),
                pltpu.VMEM((SLOTS, gate, skips), w_skip.dtype),
                pltpu.SemaphoreType.DMA((SLOTS, 4)),
                pltpu.SemaphoreType.DMA,
                pltpu.SemaphoreType.DMA,
                pltpu.SemaphoreType.DMA((repeats, cycle)),
                pltpu.SemaphoreType.DMA((repeats, cycle)),
            ],
            compiler_params=pltpu.CompilerParams(collective_id=0, has_side_effects=True, vmem_limit_bytes=46 * 2 ** 20),
        )(x_seq, w_past.reshape(layers, ch, wide), w_now.reshape(layers, ch, wide), jnp.transpose(b_conv, (1, 0, 2)),
          w_res.reshape(layers, gate, ch), w_skip.reshape(layers, gate, skips))
        return pl.pallas_call(
            _head,
            name="head",
            out_shape=(jax.ShapeDtypeStruct((rows, classes), jnp.float32), jax.ShapeDtypeStruct((rows, ch), x_seq.dtype)),
            in_specs=[vmem] * 6,
            out_specs=(vmem, vmem),
        )(skip, h, w_out1, b_out1.reshape(1, -1), w_out2, b_out2.reshape(1, -1))

    return jax.shard_map(
        local_stack,
        mesh=mesh,
        in_specs=(row_spec, P(), P(), P(), P(), P(), P(), P(), P(), P()),
        out_specs=(row_spec, row_spec),
        check_vma=False,
    )
```

```python
import functools

import jax
import jax.numpy as jnp
from jax import lax
from jax.experimental import pallas as pl
from jax.experimental.pallas import tpu as pltpu
from jax.sharding import PartitionSpec as P

TILE = 16
SLOTS = 5
SIDE = 256
SPLIT = (0, 1, 2, 3, 4, 5, 6, 7, 8, 9)
EARLY = 0


def _kernel(n_sp, repeats, cycle, rows, x_ref, wp_ref, wn_ref, b_ref, wr_ref, ws_ref,
            skip, h_ref, *scratch):
    hb, (g_s, b_s, wpb, wnb, wrb, wsb, wsem, xsem, bsem, send_sem, recv_sem) = scratch[:cycle], scratch[cycle:]
    me = lax.axis_index("sp")
    layers = repeats * cycle
    ch = x_ref.shape[1]
    gate = wn_ref.shape[2] // 2
    half = rows // 2
    pads = [max(TILE, 2 ** k) for k in range(cycle)]

    def weight_copies(layer, slot):
        pairs = ((wn_ref, wnb), (wp_ref, wpb), (wr_ref, wrb), (ws_ref, wsb))
        return [pltpu.make_async_copy(src.at[layer], dst.at[slot], wsem.at[slot, i]) for i, (src, dst) in enumerate(pairs)]

    def halo_copies(s, k):
        parts = [(pads[k] - half, half), (0, half)] if pads[k] > half else [(0, pads[k])]
        return [pltpu.make_async_remote_copy(
            src_ref=hb[k].at[s, rows + lo:rows + lo + n, :], dst_ref=hb[k].at[s, lo:lo + n, :],
            send_sem=send_sem.at[s, k, i], recv_sem=recv_sem.at[s, k, i],
            device_id={"sp": jnp.minimum(me + 1, n_sp - 1)}, device_id_type=pl.DeviceIdType.MESH) for i, (lo, n) in enumerate(parts)]

    def stack(s, carry):
        for k in range(cycle):
            layer, slot, d = s * cycle + k, k % SLOTS, 2 ** k
            after = (s, k + 1) if k + 1 < cycle else (s + 1, 0)
            old, new = hb[k].at[s], hb[after[1]].at[after[0]]
            pad, new_pad = pads[k], pads[after[1]]

            def send(part):
                ok = me < n_sp - 1
                if k + 1 == cycle:
                    ok &= s < repeats - 1
                pl.when(ok)(lambda: halo_copies(*after)[part].start())

            def receive(part):
                pl.when(me > 0)(lambda: halo_copies(s, k)[part].wait_recv())

            def fetch():
                for c in weight_copies(layer + SLOTS - 1, (k + SLOTS - 1) % SLOTS):
                    c.start()
            if k + SLOTS - 1 < cycle:
                fetch()
            else:
                pl.when(s < repeats - 1)(fetch)
            for c in weight_copies(layer, slot):
                c.wait()

            def both(buf, j):
                ca, ct = j * SIDE, gate + j * SIDE
                return jnp.concatenate([buf[slot, :, ca:ca + SIDE], buf[slot, :, ct:ct + SIDE]], axis=1)

            def now(lo, n, j):
                return jnp.dot(old[pad + lo:pad + lo + n, :], both(wnb, j), preferred_element_type=jnp.float32)

            def past(lo, n, j):
                if d < TILE:
                    rows_in = old[pad + lo - TILE:pad + lo + n, :][TILE - d:TILE - d + n, :]
                else:
                    rows_in = old[pad + lo - d:pad + lo - d + n, :]
                return jnp.dot(rows_in, both(wpb, j), preferred_element_type=jnp.float32)

            def gated(lo, n, j, z):
                ca, ct = j * SIDE, gate + j * SIDE
                a = jnp.tanh(z[:, :SIDE] + b_s[k, pl.ds(s, 1), ca:ca + SIDE])
                t = jnp.tanh(0.5 * (z[:, SIDE:] + b_s[k, pl.ds(s, 1), ct:ct + SIDE]))
                g_s[lo:lo + n, ca:ca + SIDE] = (a * (0.5 * t + 0.5)).astype(jnp.bfloat16)

            def residual(lo, n):
                res = jnp.dot(g_s[lo:lo + n, :], wrb[slot], preferred_element_type=jnp.float32)
                new[new_pad + lo:new_pad + lo + n, :] = (old[pad + lo:pad + lo + n, :].astype(jnp.float32) + res).astype(new.dtype)

            if k in SPLIT:
                zn = [now(half, half, j) for j in range(2)]
                if d > half:
                    receive(0)
                for j in range(2):
                    gated(half, half, j, past(half, half, j) + zn[j])
                residual(half, half)
                zn = [now(0, half, j) for j in range(2)]
                send(0)
                receive(1 if d > half else 0)
                for j in range(2):
                    gated(0, half, j, past(0, half, j) + zn[j])
                residual(0, half)
                for lo in (half, 0):
                    skip[lo:lo + half, :] += jnp.dot(g_s[lo:lo + half, :], wsb[slot], preferred_element_type=jnp.float32)
                if new_pad > half:
                    send(1)
            else:
                zn = [now(0, rows, j) for j in range(EARLY if k == cycle - 1 else 0)]
                for i in range(2 if d > half else 1):
                    receive(i)
                for j in range(2):
                    gated(0, rows, j, past(0, rows, j) + (zn[j] if j < len(zn) else now(0, rows, j)))
                residual(0, rows)
                for lo in (half, 0):
                    skip[lo:lo + half, :] += jnp.dot(g_s[lo:lo + half, :], wsb[slot], preferred_element_type=jnp.float32)
                for i in range(2 if new_pad > half else 1):
                    send(i)
        return carry

    x_copy = pltpu.make_async_copy(x_ref, hb[0].at[0, pads[0]:pads[0] + rows, :], xsem)
    b_copy = pltpu.make_async_copy(b_ref, b_s, bsem)
    x_copy.start()
    first = weight_copies(0, 0)
    for c in first:
        c.start()
    b_copy.start()
    barrier = pltpu.get_barrier_semaphore()

    @pl.when(me > 0)
    def _():
        pl.semaphore_signal(barrier, inc=1, device_id={"sp": me - 1}, device_id_type=pl.DeviceIdType.MESH)

    @pl.when(me == 0)
    def _():
        for s in range(repeats):
            for k in range(cycle):
                hb[k][s, 0:pads[k], :] = jnp.zeros((pads[k], ch), hb[k].dtype)

    skip[...] = jnp.zeros_like(skip)
    for layer in range(1, SLOTS - 1):
        for c in weight_copies(layer, layer):
            c.start()
    x_copy.wait()

    @pl.when(me < n_sp - 1)
    def _():
        pl.semaphore_wait(barrier, 1)
        halo_copies(0, 0)[0].start()
    b_copy.wait()
    lax.fori_loop(0, repeats, stack, 0)
    h_ref[...] = hb[0][repeats, pads[0]:pads[0] + rows, :]

    @pl.when(me < n_sp - 1)
    def _():
        for s in range(repeats):
            for k in range(cycle):
                for c in halo_copies(s, k):
                    c.wait_send()


def _head(skip, h_ref, w1_ref, c1_ref, w2_ref, c2_ref, y_ref, out_ref, y_s, ysem, hsem):
    h_copy = pltpu.make_async_copy(h_ref, out_ref, hsem)
    h_copy.start()
    half = y_s.shape[0] // 2
    copies = []
    for i in range(2):
        part = slice(i * half, (i + 1) * half)
        act = jnp.maximum(skip[part, :], 0.0).astype(jnp.bfloat16)
        mid = jnp.dot(act, w1_ref[...], preferred_element_type=jnp.float32) + c1_ref[...]
        mid = jnp.maximum(mid, 0.0).astype(jnp.bfloat16)
        y_s[part, :] = jnp.dot(mid, w2_ref[...], preferred_element_type=jnp.float32) + c2_ref[...]
        copies.append(pltpu.make_async_copy(y_s.at[part, :], y_ref.at[part, :], ysem.at[i]))
        copies[-1].start()
    for c in copies + [h_copy]:
        c.wait()


def solution(mesh):
    n_sp = mesh.shape["sp"]
    row_spec = P(("ens", "sp"), None)

    def local_stack(x_seq, w_past, w_now, b_conv, w_res, w_skip, w_out1, b_out1, w_out2, b_out2):
        repeats, cycle, ch, wide = w_past.shape
        layers, rows = repeats * cycle, x_seq.shape[0]
        gate, skips = w_res.shape[2], w_skip.shape[3]
        classes = w_out2.shape[1]
        pads = [max(TILE, 2 ** k) for k in range(cycle)]
        hbm = pl.BlockSpec(memory_space=pltpu.HBM)
        vmem = pl.BlockSpec(memory_space=pltpu.VMEM)
        skip, h = pl.pallas_call(
            functools.partial(_kernel, n_sp, repeats, cycle, rows),
            name="stack",
            out_shape=(jax.ShapeDtypeStruct((rows, skips), jnp.float32), jax.ShapeDtypeStruct((rows, ch), x_seq.dtype)),
            in_specs=[hbm] * 6,
            out_specs=(vmem, vmem),
            scratch_shapes=[
                *[pltpu.VMEM((repeats + (k == 0), pads[k] + rows, ch), x_seq.dtype) for k in range(cycle)],
                pltpu.VMEM((rows, gate), jnp.bfloat16),
                pltpu.VMEM((cycle, repeats, wide), jnp.float32),
                pltpu.VMEM((SLOTS, ch, wide), w_past.dtype),
                pltpu.VMEM((SLOTS, ch, wide), w_now.dtype),
                pltpu.VMEM((SLOTS, gate, ch), w_res.dtype),
                pltpu.VMEM((SLOTS, gate, skips), w_skip.dtype),
                pltpu.SemaphoreType.DMA((SLOTS, 4)),
                pltpu.SemaphoreType.DMA,
                pltpu.SemaphoreType.DMA,
                pltpu.SemaphoreType.DMA((repeats, cycle, 2)),
                pltpu.SemaphoreType.DMA((repeats, cycle, 2)),
            ],
            compiler_params=pltpu.CompilerParams(collective_id=0, has_side_effects=True, vmem_limit_bytes=46 * 2 ** 20),
        )(pltpu.with_memory_space_constraint(x_seq, pltpu.HBM), w_past.reshape(layers, ch, wide), w_now.reshape(layers, ch, wide), pltpu.with_memory_space_constraint(jnp.transpose(b_conv, (1, 0, 2)), pltpu.HBM),
          w_res.reshape(layers, gate, ch), w_skip.reshape(layers, gate, skips))
        return pl.pallas_call(
            _head,
            name="head",
            out_shape=(jax.ShapeDtypeStruct((rows, classes), jnp.float32), jax.ShapeDtypeStruct((rows, ch), x_seq.dtype)),
            in_specs=[vmem, vmem, vmem, vmem, vmem, vmem],
            out_specs=(hbm, hbm),
            scratch_shapes=[pltpu.VMEM((rows, classes), jnp.float32), pltpu.SemaphoreType.DMA((2,)), pltpu.SemaphoreType.DMA],
            compiler_params=pltpu.CompilerParams(vmem_limit_bytes=8 * 2 ** 20),
        )(skip, h, w_out1, b_out1.reshape(1, -1), w_out2, b_out2.reshape(1, -1))

    return jax.shard_map(
        local_stack,
        mesh=mesh,
        in_specs=(row_spec, P(), P(), P(), P(), P(), P(), P(), P(), P()),
        out_specs=(row_spec, row_spec),
        check_vma=False,
    )
```

```python
import functools

import jax
import jax.numpy as jnp
from jax import lax
from jax.experimental import pallas as pl
from jax.experimental.pallas import tpu as pltpu
from jax.sharding import PartitionSpec as P

TILE = 16
SLOTS = 5
SIDE = 256


def _kernel(n_sp, repeats, cycle, rows, x_ref, wp_ref, wn_ref, b_ref, wr_ref, ws_ref,
            skip, h_ref, *scratch):
    hb, (g_s, b_s, wpb, wnb, wrb, wsb, wsem, xsem, bsem, send_sem, recv_sem) = scratch[:cycle], scratch[cycle:]
    me = lax.axis_index("sp")
    layers = repeats * cycle
    ch = x_ref.shape[1]
    gate = wn_ref.shape[2] // 2
    half = rows // 2
    pads = [max(TILE, 2 ** k) for k in range(cycle)]

    def weight_copies(layer, slot):
        pairs = ((wn_ref, wnb), (wp_ref, wpb), (wr_ref, wrb), (ws_ref, wsb))
        return [pltpu.make_async_copy(src.at[layer], dst.at[slot], wsem.at[slot, i]) for i, (src, dst) in enumerate(pairs)]

    def halo_copies(s, k):
        parts = [(pads[k] - half, half), (0, half)] if pads[k] > half else [(0, pads[k])]
        return [pltpu.make_async_remote_copy(
            src_ref=hb[k].at[s, rows + lo:rows + lo + n, :], dst_ref=hb[k].at[s, lo:lo + n, :],
            send_sem=send_sem.at[s, k, i], recv_sem=recv_sem.at[s, k, i],
            device_id={"sp": jnp.minimum(me + 1, n_sp - 1)}, device_id_type=pl.DeviceIdType.MESH) for i, (lo, n) in enumerate(parts)]

    def stack(s, carry):
        for k in range(cycle):
            layer, slot, d = s * cycle + k, k % SLOTS, 2 ** k
            after = (s, k + 1) if k + 1 < cycle else (s + 1, 0)
            old, new = hb[k].at[s], hb[after[1]].at[after[0]]
            pad, new_pad = pads[k], pads[after[1]]

            def send(part):
                ok = me < n_sp - 1
                if k + 1 == cycle:
                    ok &= s < repeats - 1
                pl.when(ok)(lambda: halo_copies(*after)[part].start())

            def receive(part):
                pl.when(me > 0)(lambda: halo_copies(s, k)[part].wait_recv())

            def fetch():
                for c in weight_copies(layer + SLOTS - 1, (k + SLOTS - 1) % SLOTS):
                    c.start()
            def always(ahead, f):
                f() if k + ahead < cycle else pl.when(s < repeats - 1)(f)

            def arrive():
                for c in weight_copies(layer + 1, (k + 1) % SLOTS):
                    c.wait()

            def both(buf, j):
                ca, ct = j * SIDE, gate + j * SIDE
                return jnp.concatenate([buf[slot, :, ca:ca + SIDE], buf[slot, :, ct:ct + SIDE]], axis=1)

            def now(lo, n, j):
                return jnp.dot(old[pad + lo:pad + lo + n, :], both(wnb, j), preferred_element_type=jnp.float32)

            def past(lo, n, w):
                if d < TILE:
                    rows_in = old[pad + lo - TILE:pad + lo + n, :][TILE - d:TILE - d + n, :]
                else:
                    rows_in = old[pad + lo - d:pad + lo - d + n, :]
                return jnp.dot(rows_in, w, preferred_element_type=jnp.float32)

            def gated(lo, n, j, z):
                ca, ct = j * SIDE, gate + j * SIDE
                a = jnp.tanh(z[:, :SIDE] + b_s[k, pl.ds(s, 1), ca:ca + SIDE])
                t = jnp.tanh(0.5 * (z[:, SIDE:] + b_s[k, pl.ds(s, 1), ct:ct + SIDE]))
                g_s[lo:lo + n, ca:ca + SIDE] = (a * (0.5 * t + 0.5)).astype(jnp.bfloat16)

            def residual(lo, n):
                res = jnp.dot(g_s[lo:lo + n, :], wrb[slot], preferred_element_type=jnp.float32)
                new[new_pad + lo:new_pad + lo + n, :] = (old[pad + lo:pad + lo + n, :].astype(jnp.float32) + res).astype(new.dtype)

            zn = [now(half, half, j) for j in range(2)]
            if d > half:
                receive(0)
            for j in range(2):
                gated(half, half, j, past(half, half, both(wpb, j)) + zn[j])
            residual(half, half)
            zn = [now(0, half, j) for j in range(2)]
            send(0)
            always(SLOTS - 1, fetch)
            receive(1 if d > half else 0)
            always(1, arrive)
            for j in range(2):
                gated(0, half, j, past(0, half, both(wpb, j)) + zn[j])
            residual(0, half)
            for lo in (half, 0):
                skip[lo:lo + half, :] += jnp.dot(g_s[lo:lo + half, :], wsb[slot], preferred_element_type=jnp.float32)
            if new_pad > half:
                send(1)
        return carry

    x_copy = pltpu.make_async_copy(x_ref, hb[0].at[0, pads[0]:pads[0] + rows, :], xsem)
    b_copy = pltpu.make_async_copy(b_ref, b_s, bsem)
    x_copy.start()
    first = weight_copies(0, 0)
    for c in first:
        c.start()
    b_copy.start()
    barrier = pltpu.get_barrier_semaphore()

    @pl.when(me > 0)
    def _():
        pl.semaphore_signal(barrier, inc=1, device_id={"sp": me - 1}, device_id_type=pl.DeviceIdType.MESH)

    @pl.when(me == 0)
    def _():
        for s in range(repeats):
            for k in range(cycle):
                hb[k][s, 0:pads[k], :] = jnp.zeros((pads[k], ch), hb[k].dtype)

    skip[...] = jnp.zeros_like(skip)
    for layer in range(1, SLOTS - 1):
        for c in weight_copies(layer, layer):
            c.start()
    x_copy.wait()

    @pl.when(me < n_sp - 1)
    def _():
        pl.semaphore_wait(barrier, 1)
        halo_copies(0, 0)[0].start()
    b_copy.wait()
    for c in first:
        c.wait()
    lax.fori_loop(0, repeats, stack, 0)
    h_ref[...] = hb[0][repeats, pads[0]:pads[0] + rows, :]

    @pl.when(me < n_sp - 1)
    def _():
        for s in range(repeats):
            for k in range(cycle):
                for c in halo_copies(s, k):
                    c.wait_send()


def _head(skip, h_ref, w1_ref, c1_ref, w2_ref, c2_ref, y_ref, out_ref, y_s, ysem, hsem):
    h_copy = pltpu.make_async_copy(h_ref, out_ref, hsem)
    h_copy.start()
    half = y_s.shape[0] // 2
    copies = []
    for i in range(2):
        part = slice(i * half, (i + 1) * half)
        act = jnp.maximum(skip[part, :], 0.0).astype(jnp.bfloat16)
        mid = jnp.dot(act, w1_ref[...], preferred_element_type=jnp.float32) + c1_ref[...]
        mid = jnp.maximum(mid, 0.0).astype(jnp.bfloat16)
        y_s[part, :] = jnp.dot(mid, w2_ref[...], preferred_element_type=jnp.float32) + c2_ref[...]
        copies.append(pltpu.make_async_copy(y_s.at[part, :], y_ref.at[part, :], ysem.at[i]))
        copies[-1].start()
    for c in copies + [h_copy]:
        c.wait()


def solution(mesh):
    n_sp = mesh.shape["sp"]
    row_spec = P(("ens", "sp"), None)

    def local_stack(x_seq, w_past, w_now, b_conv, w_res, w_skip, w_out1, b_out1, w_out2, b_out2):
        repeats, cycle, ch, wide = w_past.shape
        layers, rows = repeats * cycle, x_seq.shape[0]
        gate, skips = w_res.shape[2], w_skip.shape[3]
        classes = w_out2.shape[1]
        pads = [max(TILE, 2 ** k) for k in range(cycle)]
        hbm = pl.BlockSpec(memory_space=pltpu.HBM)
        vmem = pl.BlockSpec(memory_space=pltpu.VMEM)
        skip, h = pl.pallas_call(
            functools.partial(_kernel, n_sp, repeats, cycle, rows),
            name="stack",
            out_shape=(jax.ShapeDtypeStruct((rows, skips), jnp.float32), jax.ShapeDtypeStruct((rows, ch), x_seq.dtype)),
            in_specs=[hbm] * 6,
            out_specs=(vmem, vmem),
            scratch_shapes=[
                *[pltpu.VMEM((repeats + (k == 0), pads[k] + rows, ch), x_seq.dtype) for k in range(cycle)],
                pltpu.VMEM((rows, gate), jnp.bfloat16),
                pltpu.VMEM((cycle, repeats, wide), jnp.float32),
                pltpu.VMEM((SLOTS, ch, wide), w_past.dtype),
                pltpu.VMEM((SLOTS, ch, wide), w_now.dtype),
                pltpu.VMEM((SLOTS, gate, ch), w_res.dtype),
                pltpu.VMEM((SLOTS, gate, skips), w_skip.dtype),
                pltpu.SemaphoreType.DMA((SLOTS, 4)),
                pltpu.SemaphoreType.DMA,
                pltpu.SemaphoreType.DMA,
                pltpu.SemaphoreType.DMA((repeats, cycle, 2)),
                pltpu.SemaphoreType.DMA((repeats, cycle, 2)),
            ],
            compiler_params=pltpu.CompilerParams(collective_id=0, has_side_effects=True, vmem_limit_bytes=46 * 2 ** 20),
        )(pltpu.with_memory_space_constraint(x_seq, pltpu.HBM), w_past.reshape(layers, ch, wide), w_now.reshape(layers, ch, wide), pltpu.with_memory_space_constraint(jnp.transpose(b_conv, (1, 0, 2)), pltpu.HBM),
          w_res.reshape(layers, gate, ch), w_skip.reshape(layers, gate, skips))
        return pl.pallas_call(
            _head,
            name="head",
            out_shape=(jax.ShapeDtypeStruct((rows, classes), jnp.float32), jax.ShapeDtypeStruct((rows, ch), x_seq.dtype)),
            in_specs=[vmem, vmem, vmem, vmem, vmem, vmem],
            out_specs=(hbm, hbm),
            scratch_shapes=[pltpu.VMEM((rows, classes), jnp.float32), pltpu.SemaphoreType.DMA((2,)), pltpu.SemaphoreType.DMA],
            compiler_params=pltpu.CompilerParams(vmem_limit_bytes=8 * 2 ** 20),
        )(skip, h, w_out1, b_out1.reshape(1, -1), w_out2, b_out2.reshape(1, -1))

    return jax.shard_map(
        local_stack,
        mesh=mesh,
        in_specs=(row_spec, P(), P(), P(), P(), P(), P(), P(), P(), P()),
        out_specs=(row_spec, row_spec),
        check_vma=False,
    )
```

```python
import functools

import jax
import jax.numpy as jnp
from jax import lax
from jax.experimental import pallas as pl
from jax.experimental.pallas import tpu as pltpu
from jax.sharding import PartitionSpec as P

TILE = 16
SLOTS = 5
SIDE = 256


def _kernel(n_sp, repeats, cycle, rows, x_ref, wp_ref, wn_ref, b_ref, wr_ref, ws_ref,
            skip, h_ref, *scratch):
    hb, (g_s, b_s, wpb, wnb, wrb, wsb, wsem, xsem, bsem, send_sem, recv_sem) = scratch[:cycle], scratch[cycle:]
    me = lax.axis_index("sp")
    layers = repeats * cycle
    ch = x_ref.shape[1]
    gate = wn_ref.shape[2] // 2
    half = rows // 2
    pads = [max(TILE, 2 ** k) for k in range(cycle)]

    def weight_copies(layer, slot):
        pairs = ((wn_ref, wnb), (wp_ref, wpb), (wr_ref, wrb), (ws_ref, wsb))
        return [pltpu.make_async_copy(src.at[layer], dst.at[slot], wsem.at[slot, i]) for i, (src, dst) in enumerate(pairs)]

    def halo_copies(s, k):
        parts = [(pads[k] - half, half), (0, half)] if pads[k] > half else [(0, pads[k])]
        return [pltpu.make_async_remote_copy(
            src_ref=hb[k].at[s, rows + lo:rows + lo + n, :], dst_ref=hb[k].at[s, lo:lo + n, :],
            send_sem=send_sem.at[s, k, i], recv_sem=recv_sem.at[s, k, i],
            device_id={"sp": jnp.minimum(me + 1, n_sp - 1)}, device_id_type=pl.DeviceIdType.MESH) for i, (lo, n) in enumerate(parts)]

    def stack(s, carry):
        for k in range(cycle):
            layer, slot, d = s * cycle + k, k % SLOTS, 2 ** k
            after = (s, k + 1) if k + 1 < cycle else (s + 1, 0)
            old, new = hb[k].at[s], hb[after[1]].at[after[0]]
            pad, new_pad = pads[k], pads[after[1]]

            def send(part):
                ok = me < n_sp - 1
                if k + 1 == cycle:
                    ok &= s < repeats - 1
                pl.when(ok)(lambda: halo_copies(*after)[part].start())

            def receive(part):
                pl.when(me > 0)(lambda: halo_copies(s, k)[part].wait_recv())

            def fetch():
                for c in weight_copies(layer + SLOTS - 1, (k + SLOTS - 1) % SLOTS):
                    c.start()
            def always(ahead, f):
                f() if k + ahead < cycle else pl.when(s < repeats - 1)(f)

            def arrive():
                for c in weight_copies(layer + 1, (k + 1) % SLOTS):
                    c.wait()

            def both(buf, j):
                ca, ct = j * SIDE, gate + j * SIDE
                return jnp.concatenate([buf[slot, :, ca:ca + SIDE], buf[slot, :, ct:ct + SIDE]], axis=1)

            def now(lo, n, j):
                return jnp.dot(old[pad + lo:pad + lo + n, :], both(wnb, j), preferred_element_type=jnp.float32)

            def past(lo, n, w):
                if d < TILE:
                    rows_in = old[pad + lo - TILE:pad + lo + n, :][TILE - d:TILE - d + n, :]
                else:
                    rows_in = old[pad + lo - d:pad + lo - d + n, :]
                return jnp.dot(rows_in, w, preferred_element_type=jnp.float32)

            def gated(lo, n, j, z):
                ca, ct = j * SIDE, gate + j * SIDE
                a = jnp.tanh(z[:, :SIDE] + b_s[k, pl.ds(s, 1), ca:ca + SIDE])
                t = jnp.tanh(0.5 * (z[:, SIDE:] + b_s[k, pl.ds(s, 1), ct:ct + SIDE]))
                g_s[lo:lo + n, ca:ca + SIDE] = (a * (0.5 * t + 0.5)).astype(jnp.bfloat16)

            def residual(lo, n):
                res = jnp.dot(g_s[lo:lo + n, :], wrb[slot], preferred_element_type=jnp.float32)
                new[new_pad + lo:new_pad + lo + n, :] = (old[pad + lo:pad + lo + n, :].astype(jnp.float32) + res).astype(new.dtype)

            zn = [now(half, half, j) for j in range(2)]
            if d > half:
                receive(0)
            for j in range(2):
                gated(half, half, j, past(half, half, both(wpb, j)) + zn[j])
            residual(half, half)
            zn = [now(0, half, j) for j in range(2)]
            send(0)
            always(SLOTS - 1, fetch)
            receive(1 if d > half else 0)
            always(1, arrive)
            for j in range(2):
                gated(0, half, j, past(0, half, both(wpb, j)) + zn[j])
            residual(0, half)
            for lo in (half, 0):
                skip[lo:lo + half, :] += jnp.dot(g_s[lo:lo + half, :], wsb[slot], preferred_element_type=jnp.float32)
            if new_pad > half:
                send(1)
        return carry

    x_copy = pltpu.make_async_copy(x_ref, hb[0].at[0, pads[0]:pads[0] + rows, :], xsem)
    b_copy = pltpu.make_async_copy(b_ref, b_s, bsem)
    first = weight_copies(0, 0)
    first[0].start()
    x_copy.start()
    b_copy.start()
    for c in first[1:]:
        c.start()
    barrier = pltpu.get_barrier_semaphore()

    @pl.when(me > 0)
    def _():
        pl.semaphore_signal(barrier, inc=1, device_id={"sp": me - 1}, device_id_type=pl.DeviceIdType.MESH)

    @pl.when(me == 0)
    def _():
        for s in range(repeats):
            for k in range(cycle):
                hb[k][s, 0:pads[k], :] = jnp.zeros((pads[k], ch), hb[k].dtype)

    skip[...] = jnp.zeros_like(skip)
    for layer in range(1, SLOTS - 1):
        for c in weight_copies(layer, layer):
            c.start()
    x_copy.wait()

    @pl.when(me < n_sp - 1)
    def _():
        pl.semaphore_wait(barrier, 1)
        halo_copies(0, 0)[0].start()
    b_copy.wait()
    for c in first:
        c.wait()
    lax.fori_loop(0, repeats, stack, 0)
    h_ref[...] = hb[0][repeats, pads[0]:pads[0] + rows, :]

    @pl.when(me < n_sp - 1)
    def _():
        for s in range(repeats):
            for k in range(cycle):
                for c in halo_copies(s, k):
                    c.wait_send()


def _head(skip, h_ref, w1_ref, c1_ref, w2_ref, c2_ref, y_ref, out_ref, y_s, ysem, hsem):
    h_copy = pltpu.make_async_copy(h_ref, out_ref, hsem)
    h_copy.start()
    half = y_s.shape[0] // 2
    copies = []
    for i in range(2):
        part = slice(i * half, (i + 1) * half)
        act = jnp.maximum(skip[part, :], 0.0).astype(jnp.bfloat16)
        mid = jnp.dot(act, w1_ref[...], preferred_element_type=jnp.float32) + c1_ref[...]
        mid = jnp.maximum(mid, 0.0).astype(jnp.bfloat16)
        y_s[part, :] = jnp.dot(mid, w2_ref[...], preferred_element_type=jnp.float32) + c2_ref[...]
        copies.append(pltpu.make_async_copy(y_s.at[part, :], y_ref.at[part, :], ysem.at[i]))
        copies[-1].start()
    for c in copies + [h_copy]:
        c.wait()


def solution(mesh):
    n_sp = mesh.shape["sp"]
    row_spec = P(("ens", "sp"), None)

    def local_stack(x_seq, w_past, w_now, b_conv, w_res, w_skip, w_out1, b_out1, w_out2, b_out2):
        repeats, cycle, ch, wide = w_past.shape
        layers, rows = repeats * cycle, x_seq.shape[0]
        gate, skips = w_res.shape[2], w_skip.shape[3]
        classes = w_out2.shape[1]
        pads = [max(TILE, 2 ** k) for k in range(cycle)]
        hbm = pl.BlockSpec(memory_space=pltpu.HBM)
        vmem = pl.BlockSpec(memory_space=pltpu.VMEM)
        skip, h = pl.pallas_call(
            functools.partial(_kernel, n_sp, repeats, cycle, rows),
            name="stack",
            out_shape=(jax.ShapeDtypeStruct((rows, skips), jnp.float32), jax.ShapeDtypeStruct((rows, ch), x_seq.dtype)),
            in_specs=[hbm] * 6,
            out_specs=(vmem, vmem),
            scratch_shapes=[
                *[pltpu.VMEM((repeats + (k == 0), pads[k] + rows, ch), x_seq.dtype) for k in range(cycle)],
                pltpu.VMEM((rows, gate), jnp.bfloat16),
                pltpu.VMEM((cycle, repeats, wide), jnp.float32),
                pltpu.VMEM((SLOTS, ch, wide), w_past.dtype),
                pltpu.VMEM((SLOTS, ch, wide), w_now.dtype),
                pltpu.VMEM((SLOTS, gate, ch), w_res.dtype),
                pltpu.VMEM((SLOTS, gate, skips), w_skip.dtype),
                pltpu.SemaphoreType.DMA((SLOTS, 4)),
                pltpu.SemaphoreType.DMA,
                pltpu.SemaphoreType.DMA,
                pltpu.SemaphoreType.DMA((repeats, cycle, 2)),
                pltpu.SemaphoreType.DMA((repeats, cycle, 2)),
            ],
            compiler_params=pltpu.CompilerParams(collective_id=0, has_side_effects=True, vmem_limit_bytes=46 * 2 ** 20),
        )(pltpu.with_memory_space_constraint(x_seq, pltpu.HBM), w_past.reshape(layers, ch, wide), w_now.reshape(layers, ch, wide), pltpu.with_memory_space_constraint(jnp.transpose(b_conv, (1, 0, 2)), pltpu.HBM),
          w_res.reshape(layers, gate, ch), w_skip.reshape(layers, gate, skips))
        return pl.pallas_call(
            _head,
            name="head",
            out_shape=(jax.ShapeDtypeStruct((rows, classes), jnp.float32), jax.ShapeDtypeStruct((rows, ch), x_seq.dtype)),
            in_specs=[vmem, vmem, vmem, vmem, vmem, vmem],
            out_specs=(hbm, hbm),
            scratch_shapes=[pltpu.VMEM((rows, classes), jnp.float32), pltpu.SemaphoreType.DMA((2,)), pltpu.SemaphoreType.DMA],
            compiler_params=pltpu.CompilerParams(vmem_limit_bytes=8 * 2 ** 20),
        )(skip, h, w_out1, b_out1.reshape(1, -1), w_out2, b_out2.reshape(1, -1))

    return jax.shard_map(
        local_stack,
        mesh=mesh,
        in_specs=(row_spec, P(), P(), P(), P(), P(), P(), P(), P(), P()),
        out_specs=(row_spec, row_spec),
        check_vma=False,
    )
```

```python
import functools

import jax
import jax.numpy as jnp
from jax import lax
from jax.experimental import pallas as pl
from jax.experimental.pallas import tpu as pltpu
from jax.sharding import PartitionSpec as P

TILE = 16
SLOTS = 5
SIDE = 256


def _kernel(n_sp, repeats, cycle, rows, x_ref, wp_ref, wn_ref, b_ref, wr_ref, ws_ref,
            skip, h_ref, *scratch):
    hb, (g_s, b_s, wpb, wnb, wrb, wsb, wsem, xsem, bsem, send_sem, recv_sem) = scratch[:cycle], scratch[cycle:]
    me = lax.axis_index("sp")
    layers = repeats * cycle
    ch = x_ref.shape[1]
    gate = wn_ref.shape[2] // 2
    half = rows // 2
    pads = [max(TILE, 2 ** k) for k in range(cycle)]

    def weight_copies(layer, slot):
        pairs = ((wn_ref, wnb), (wp_ref, wpb), (wr_ref, wrb), (ws_ref, wsb))
        return [pltpu.make_async_copy(src.at[layer], dst.at[slot], wsem.at[slot, i]) for i, (src, dst) in enumerate(pairs)]

    def halo_copies(s, k):
        parts = [(pads[k] - half, half), (0, half)] if pads[k] > half else [(0, pads[k])]
        return [pltpu.make_async_remote_copy(
            src_ref=hb[k].at[s, rows + lo:rows + lo + n, :], dst_ref=hb[k].at[s, lo:lo + n, :],
            send_sem=send_sem.at[s, k, i], recv_sem=recv_sem.at[s, k, i],
            device_id={"sp": jnp.minimum(me + 1, n_sp - 1)}, device_id_type=pl.DeviceIdType.MESH) for i, (lo, n) in enumerate(parts)]

    def stack(s, carry):
        for k in range(cycle):
            layer, slot, d = s * cycle + k, k % SLOTS, 2 ** k
            after = (s, k + 1) if k + 1 < cycle else (s + 1, 0)
            old, new = hb[k].at[s], hb[after[1]].at[after[0]]
            pad, new_pad = pads[k], pads[after[1]]

            def send(part):
                ok = me < n_sp - 1
                if k + 1 == cycle:
                    ok &= s < repeats - 1
                pl.when(ok)(lambda: halo_copies(*after)[part].start())

            def receive(part):
                pl.when(me > 0)(lambda: halo_copies(s, k)[part].wait_recv())

            def fetch():
                for c in weight_copies(layer + SLOTS - 1, (k + SLOTS - 1) % SLOTS):
                    c.start()
            def always(ahead, f):
                f() if k + ahead < cycle else pl.when(s < repeats - 1)(f)

            def arrive():
                for c in weight_copies(layer + 1, (k + 1) % SLOTS):
                    c.wait()

            def both(buf, j):
                ca, ct = j * SIDE, gate + j * SIDE
                return jnp.concatenate([buf[slot, :, ca:ca + SIDE], buf[slot, :, ct:ct + SIDE]], axis=1)

            def now(lo, n, j):
                return jnp.dot(old[pad + lo:pad + lo + n, :], both(wnb, j), preferred_element_type=jnp.float32)

            def past(lo, n, w):
                if d < TILE:
                    rows_in = old[pad + lo - TILE:pad + lo + n, :][TILE - d:TILE - d + n, :]
                else:
                    rows_in = old[pad + lo - d:pad + lo - d + n, :]
                return jnp.dot(rows_in, w, preferred_element_type=jnp.float32)

            def gated(lo, n, j, z):
                ca, ct = j * SIDE, gate + j * SIDE
                a = jnp.tanh(z[:, :SIDE] + b_s[k, pl.ds(s, 1), ca:ca + SIDE])
                t = jnp.tanh(0.5 * (z[:, SIDE:] + b_s[k, pl.ds(s, 1), ct:ct + SIDE]))
                g_s[lo:lo + n, ca:ca + SIDE] = (a * (0.5 * t + 0.5)).astype(jnp.bfloat16)

            def residual(lo, n):
                res = jnp.dot(g_s[lo:lo + n, :], wrb[slot], preferred_element_type=jnp.float32)
                new[new_pad + lo:new_pad + lo + n, :] = (old[pad + lo:pad + lo + n, :].astype(jnp.float32) + res).astype(new.dtype)

            zn = [now(half, half, j) for j in range(2)]
            if d > half:
                receive(0)
            for j in range(2):
                gated(half, half, j, past(half, half, both(wpb, j)) + zn[j])
            residual(half, half)
            zn = [now(0, half, j) for j in range(2)]
            send(0)
            always(SLOTS - 1, fetch)
            receive(1 if d > half else 0)
            always(1, arrive)
            for j in range(2):
                gated(0, half, j, past(0, half, both(wpb, j)) + zn[j])
            residual(0, half)
            for lo in (half, 0):
                skip[lo:lo + half, :] += jnp.dot(g_s[lo:lo + half, :], wsb[slot], preferred_element_type=jnp.float32)
            if new_pad > half:
                send(1)
        return carry

    x_copy = pltpu.make_async_copy(x_ref, hb[0].at[0, pads[0]:pads[0] + rows, :], xsem)
    b_copy = pltpu.make_async_copy(b_ref, b_s, bsem)
    first = weight_copies(0, 0)
    first[0].start()
    x_copy.start()
    b_copy.start()
    for c in first[1:]:
        c.start()
    barrier = pltpu.get_barrier_semaphore()

    @pl.when(me > 0)
    def _():
        pl.semaphore_signal(barrier, inc=1, device_id={"sp": me - 1}, device_id_type=pl.DeviceIdType.MESH)

    @pl.when(me == 0)
    def _():
        for s in range(repeats):
            for k in range(cycle):
                hb[k][s, 0:pads[k], :] = jnp.zeros((pads[k], ch), hb[k].dtype)

    skip[...] = jnp.zeros_like(skip)
    for layer in range(1, SLOTS - 1):
        for c in weight_copies(layer, layer):
            c.start()
    x_copy.wait()

    @pl.when(me < n_sp - 1)
    def _():
        pl.semaphore_wait(barrier, 1)
        halo_copies(0, 0)[0].start()
    b_copy.wait()
    for c in first:
        c.wait()
    lax.fori_loop(0, repeats, stack, 0)
    h_ref[...] = hb[0][repeats, pads[0]:pads[0] + rows, :]

    @pl.when(me < n_sp - 1)
    def _():
        for s in range(repeats):
            for k in range(cycle):
                for c in halo_copies(s, k):
                    c.wait_send()


def _head(skip, h_ref, w1_ref, c1_ref, w2_ref, c2_ref, y_ref, out_ref, y_s, ysem, hsem):
    h_copy = pltpu.make_async_copy(h_ref, out_ref, hsem)
    h_copy.start()
    part_rows = y_s.shape[0] // 4
    copies = []
    for i in range(4):
        part = slice(i * part_rows, (i + 1) * part_rows)
        act = jnp.maximum(skip[part, :], 0.0).astype(jnp.bfloat16)
        mid = jnp.dot(act, w1_ref[...], preferred_element_type=jnp.float32) + c1_ref[...]
        mid = jnp.maximum(mid, 0.0).astype(jnp.bfloat16)
        y_s[part, :] = jnp.dot(mid, w2_ref[...], preferred_element_type=jnp.float32) + c2_ref[...]
        copies.append(pltpu.make_async_copy(y_s.at[part, :], y_ref.at[part, :], ysem.at[i]))
        copies[-1].start()
    for c in copies + [h_copy]:
        c.wait()


def solution(mesh):
    n_sp = mesh.shape["sp"]
    row_spec = P(("ens", "sp"), None)

    def local_stack(x_seq, w_past, w_now, b_conv, w_res, w_skip, w_out1, b_out1, w_out2, b_out2):
        repeats, cycle, ch, wide = w_past.shape
        layers, rows = repeats * cycle, x_seq.shape[0]
        gate, skips = w_res.shape[2], w_skip.shape[3]
        classes = w_out2.shape[1]
        pads = [max(TILE, 2 ** k) for k in range(cycle)]
        hbm = pl.BlockSpec(memory_space=pltpu.HBM)
        vmem = pl.BlockSpec(memory_space=pltpu.VMEM)
        skip, h = pl.pallas_call(
            functools.partial(_kernel, n_sp, repeats, cycle, rows),
            name="stack",
            out_shape=(jax.ShapeDtypeStruct((rows, skips), jnp.float32), jax.ShapeDtypeStruct((rows, ch), x_seq.dtype)),
            in_specs=[hbm] * 6,
            out_specs=(vmem, vmem),
            scratch_shapes=[
                *[pltpu.VMEM((repeats + (k == 0), pads[k] + rows, ch), x_seq.dtype) for k in range(cycle)],
                pltpu.VMEM((rows, gate), jnp.bfloat16),
                pltpu.VMEM((cycle, repeats, wide), jnp.float32),
                pltpu.VMEM((SLOTS, ch, wide), w_past.dtype),
                pltpu.VMEM((SLOTS, ch, wide), w_now.dtype),
                pltpu.VMEM((SLOTS, gate, ch), w_res.dtype),
                pltpu.VMEM((SLOTS, gate, skips), w_skip.dtype),
                pltpu.SemaphoreType.DMA((SLOTS, 4)),
                pltpu.SemaphoreType.DMA,
                pltpu.SemaphoreType.DMA,
                pltpu.SemaphoreType.DMA((repeats, cycle, 2)),
                pltpu.SemaphoreType.DMA((repeats, cycle, 2)),
            ],
            compiler_params=pltpu.CompilerParams(collective_id=0, has_side_effects=True, vmem_limit_bytes=46 * 2 ** 20),
        )(pltpu.with_memory_space_constraint(x_seq, pltpu.HBM), w_past.reshape(layers, ch, wide), w_now.reshape(layers, ch, wide), pltpu.with_memory_space_constraint(jnp.transpose(b_conv, (1, 0, 2)), pltpu.HBM),
          w_res.reshape(layers, gate, ch), w_skip.reshape(layers, gate, skips))
        return pl.pallas_call(
            _head,
            name="head",
            out_shape=(jax.ShapeDtypeStruct((rows, classes), jnp.float32), jax.ShapeDtypeStruct((rows, ch), x_seq.dtype)),
            in_specs=[vmem, vmem, vmem, vmem, vmem, vmem],
            out_specs=(hbm, hbm),
            scratch_shapes=[pltpu.VMEM((rows, classes), jnp.float32), pltpu.SemaphoreType.DMA((4,)), pltpu.SemaphoreType.DMA],
            compiler_params=pltpu.CompilerParams(vmem_limit_bytes=8 * 2 ** 20),
        )(skip, h, w_out1, b_out1.reshape(1, -1), w_out2, b_out2.reshape(1, -1))

    return jax.shard_map(
        local_stack,
        mesh=mesh,
        in_specs=(row_spec, P(), P(), P(), P(), P(), P(), P(), P(), P()),
        out_specs=(row_spec, row_spec),
        check_vma=False,
    )
```
